32 devices in a mesh: dp: 1 (over z), sp: 32 (over y, x, core).
Axes of the slice: x: 4, y: 4, z: 1, core: 2. Of those that a mesh axis runs over, the one named last changes fastest.
The devices are a block of a 4x4x8 slice.
Arguments:
- signal: bfloat16 [65536, 2560], P(('dp', 'sp'))
- w_first: bfloat16 [10, 1024, 2, 64, 64], P(None, 'sp')
- w_second: bfloat16 [10, 1024, 2, 64, 64], P(None, 'sp')
Outputs:
- output: bfloat16 [65536, 2560], P(('dp', 'sp'))
All inputs are finite; a program needn't handle non-finite values.
Results may differ from the reference program's by a relative error of at most 0.02.
Values are sent between devices in bfloat16 or wider.
A program may use at most 768 MiB of HBM per device.

```python
import jax
import jax.numpy as jnp
import math
from jax import lax

SEQ_LEN = 65536
CHANNELS = 2560
BLOCK_SIZE = 64

NUM_BLOCKS = SEQ_LEN // BLOCK_SIZE
STAGES = int(math.log2(NUM_BLOCKS))


def setup_inputs(seed: int = 0, part: int = 0) -> dict:
    key_signal = jax.random.fold_in(jax.random.key(seed + 1), part)
    key_first = jax.random.key(seed + 2)
    key_second = jax.random.key(seed + 3)
    w_shape = (STAGES, NUM_BLOCKS, 2, BLOCK_SIZE, BLOCK_SIZE)
    w_scale = (2 * BLOCK_SIZE) ** -0.5
    signal = jax.random.normal(key_signal, (SEQ_LEN, CHANNELS), jnp.float32)
    w_first = jax.random.normal(key_first, w_shape, jnp.float32) * w_scale
    w_second = jax.random.normal(key_second, w_shape, jnp.float32) * w_scale
    return {"signal": signal.astype(jnp.bfloat16), "w_first": w_first.astype(jnp.bfloat16), "w_second": w_second.astype(jnp.bfloat16)}


def butterfly_stage(act_blocks, weights, distance):
    grouped = act_blocks.reshape(NUM_BLOCKS // (2 * distance), 2, distance, BLOCK_SIZE, act_blocks.shape[2])
    partner = grouped[:, ::-1].reshape(act_blocks.shape)
    paired = jnp.stack([act_blocks, partner], axis=1).astype(jnp.float32)
    mixed = jnp.einsum("ltij,ltjc->lic", weights.astype(jnp.float32), paired)
    return mixed.astype(jnp.bfloat16)


def apply_map(act_blocks, weights, distances):
    for stage, distance in enumerate(distances):
        act_blocks = butterfly_stage(act_blocks, weights[stage], distance)
    return act_blocks


def reference(signal, w_first, w_second):
    col_width = min(CHANNELS, 128)
    col_groups = CHANNELS // col_width
    grouped = signal.reshape(NUM_BLOCKS, BLOCK_SIZE, col_groups, col_width).transpose(2, 0, 1, 3)
    dist_down = [2 ** (STAGES - 1 - level) for level in range(STAGES)]
    dist_up = [2 ** level for level in range(STAGES)]

    def one_group(act_blocks):
        hidden = apply_map(act_blocks, w_first, dist_down)
        hidden = jax.nn.gelu(hidden.astype(jnp.float32), approximate=False).astype(jnp.bfloat16)
        return apply_map(hidden, w_second, dist_up)

    mapped = lax.map(one_group, grouped)
    return mapped.transpose(1, 2, 0, 3).reshape(SEQ_LEN, CHANNELS)
```

```python
import functools

import jax
import jax.numpy as jnp
from jax import lax
from jax.experimental import pallas as pl
from jax.experimental.pallas import tpu as pltpu
from jax.sharding import PartitionSpec as P

MESH = pl.DeviceIdType.MESH
CHUNKS = 5
UNROLL = 4


def gelu(x):
    return 0.5 * x * (1.0 + lax.erf(x * (0.5 ** 0.5)))


def stage(src, dst, weights, s, dist, activate=False):
    blocks, rows, _ = src.shape

    def pairs(group, carry):
        for member in range(UNROLL):
            pair = group * UNROLL + member
            low = (pair // dist) * (2 * dist) + pair % dist
            high = low + dist
            mat = jnp.concatenate([weights[s, low], weights[s, high]], axis=0)
            act = jnp.concatenate([src[low], src[high]], axis=0)
            mixed = jnp.dot(mat, act, preferred_element_type=jnp.float32).astype(jnp.bfloat16)
            if activate:
                mixed = gelu(mixed.astype(jnp.float32)).astype(jnp.bfloat16)
            dst[low] = mixed[:rows]
            dst[high] = mixed[rows:]
        return carry

    lax.fori_loop(0, blocks // 2 // UNROLL, pairs, 0)


def kernel(n, signal, rows_first, rows_second, out, buf1, buf2, buf3, ping, pong,
           far_first, far_second, near_first, near_second, send_sems, recv_sems, wsend_sems, wrecv_sems, near_sems):
    me = lax.axis_index("sp")
    far = far_first.shape[0]
    chunks, blocks, block_rows, width = buf1.shape

    near1 = pltpu.make_async_copy(rows_first.at[pl.ds(far, far)], near_first, near_sems.at[0])
    near2 = pltpu.make_async_copy(rows_second.at[pl.ds(0, far)], near_second, near_sems.at[1])
    near1.start()
    near2.start()

    barrier = pltpu.get_barrier_semaphore()

    def greet(k, carry):
        pl.semaphore_signal(barrier, inc=1, device_id={"sp": lax.rem(me + k, n)}, device_id_type=MESH)
        return carry

    lax.fori_loop(1, n, greet, 0)
    pl.semaphore_wait(barrier, n - 1)

    def spread(src_of, dst, send_sem, recv_sem):
        def one(k, carry):
            peer = lax.rem(me + k, n)
            pltpu.make_async_remote_copy(
                src_ref=src_of(peer), dst_ref=dst, send_sem=send_sem, recv_sem=recv_sem,
                device_id={"sp": peer}, device_id_type=MESH).start()
            return carry

        lax.fori_loop(1, n, one, 0)

    def wait_bytes(ref, sem):
        pltpu.make_async_copy(ref, ref, sem).wait()

    def rows_of(block):
        return pl.ds(pl.multiple_of(block * block_rows, block_rows), block_rows)

    def columns_of(chunk):
        return pl.ds(pl.multiple_of(chunk * width, width), width)

    def send_signal(chunk, carry):
        cols = columns_of(chunk)
        spread(lambda peer: signal.at[rows_of(peer), cols], buf1.at[chunk, me], send_sems.at[0, chunk], recv_sems.at[0, chunk])
        pltpu.make_async_copy(signal.at[rows_of(me), cols], buf1.at[chunk, me], recv_sems.at[0, chunk]).start()
        return carry

    def send_weights(rows, base, dst, slot):
        spread(lambda peer: rows.at[pl.ds(base, far), peer], dst.at[:, me], wsend_sems.at[slot], wrecv_sems.at[slot])
        pltpu.make_async_copy(rows.at[pl.ds(base, far), me], dst.at[:, me], wrecv_sems.at[slot]).start()

    send_signal(0, 0)
    send_weights(rows_first, 0, far_first, 0)
    lax.fori_loop(1, chunks, send_signal, 0)
    send_weights(rows_second, far, far_second, 1)

    def exchange(chunk, src, dst, phase):
        spread(lambda peer: src.at[chunk, peer], dst.at[chunk, me], send_sems.at[phase, chunk], recv_sems.at[phase, chunk])
        dst[chunk, me] = src[chunk, me]

    wait_bytes(far_first, wrecv_sems.at[0])

    def first_far(chunk, carry):
        wait_bytes(buf1.at[chunk], recv_sems.at[0, chunk])
        refs = [buf1.at[chunk]] + [(ping, pong)[s % 2] for s in range(far - 1)] + [buf1.at[chunk]]
        for s in range(far):
            stage(refs[s], refs[s + 1], far_first, s, 2 ** (far - 1 - s))
        exchange(chunk, buf1, buf2, 1)
        return carry

    lax.fori_loop(0, chunks, first_far, 0)
    near1.wait()
    near2.wait()

    def middle(chunk, carry):
        wait_bytes(buf2.at[chunk, pl.ds(0, n - 1)], recv_sems.at[1, chunk])
        refs = [buf2.at[chunk]] + [(ping, pong)[s % 2] for s in range(2 * far - 1)] + [buf2.at[chunk]]
        for s in range(far):
            stage(refs[s], refs[s + 1], near_first, s, 2 ** (far - 1 - s), activate=s == far - 1)
        for s in range(far):
            stage(refs[far + s], refs[far + s + 1], near_second, s, 2 ** s)
        exchange(chunk, buf2, buf3, 2)
        return carry

    lax.fori_loop(0, chunks, middle, 0)
    wait_bytes(far_second, wrecv_sems.at[1])

    def second_far(chunk, carry):
        wait_bytes(buf3.at[chunk, pl.ds(0, n - 1)], recv_sems.at[2, chunk])
        refs = [buf3.at[chunk]] + [(ping, pong)[s % 2] for s in range(far - 1)] + [buf3.at[chunk]]
        for s in range(far):
            stage(refs[s], refs[s + 1], far_second, s, 2 ** s)
        dst = out.at[rows_of(me), columns_of(chunk)]
        spread(lambda peer: buf3.at[chunk, peer], dst, send_sems.at[3, chunk], recv_sems.at[3, chunk])
        pltpu.make_async_copy(buf3.at[chunk, me], dst, recv_sems.at[3, chunk]).start()
        return carry

    lax.fori_loop(0, chunks, second_far, 0)

    def finish(chunk, carry):
        wait_bytes(out.at[:, columns_of(chunk)], recv_sems.at[3, chunk])
        for phase in range(4):
            wait_bytes(buf1.at[chunk, pl.ds(0, n - 1)], send_sems.at[phase, chunk])
        return carry

    lax.fori_loop(0, chunks, finish, 0)
    for slot in range(2):
        wait_bytes(far_first.at[:, pl.ds(0, n - 1)], wsend_sems.at[slot])


def solution(mesh):
    n = mesh.shape["sp"]

    def weight_rows(weights, distances):
        stages, blocks, two, size, _ = weights.shape
        block = lax.axis_index("sp") * blocks + jnp.arange(blocks)
        upper = (block[None, :] // jnp.array(distances)[:, None]) % 2 == 1
        own_first = jnp.concatenate([weights[:, :, 0], weights[:, :, 1]], axis=-1)
        own_last = jnp.concatenate([weights[:, :, 1], weights[:, :, 0]], axis=-1)
        return jnp.where(upper[:, :, None, None], own_last, own_first)

    def device_program(signal, w_first, w_second):
        stages, blocks, _, block_rows, _ = w_first.shape
        far = stages // 2
        width = signal.shape[1] // CHUNKS
        dist_down = [2 ** (stages - 1 - level) for level in range(stages)]
        rows_first = weight_rows(w_first, dist_down)
        rows_second = weight_rows(w_second, dist_down[::-1])
        buf = pltpu.VMEM((CHUNKS, blocks, block_rows, width), jnp.bfloat16)
        half = pltpu.VMEM((blocks, block_rows, width), jnp.bfloat16)
        mats = pltpu.VMEM((far, blocks, block_rows, 2 * block_rows), jnp.bfloat16)
        return pl.pallas_call(
            functools.partial(kernel, n),
            out_shape=jax.ShapeDtypeStruct(signal.shape, signal.dtype),
            in_specs=[pl.BlockSpec(memory_space=pl.ANY)] * 3,
            out_specs=pl.BlockSpec(memory_space=pl.ANY),
            scratch_shapes=[buf, buf, buf, half, half, mats, mats, mats, mats,
                            pltpu.SemaphoreType.DMA((4, CHUNKS)), pltpu.SemaphoreType.DMA((4, CHUNKS)),
                            pltpu.SemaphoreType.DMA((2,)), pltpu.SemaphoreType.DMA((2,)), pltpu.SemaphoreType.DMA((2,))],
            compiler_params=pltpu.CompilerParams(collective_id=0, has_side_effects=True, vmem_limit_bytes=62 * 1024 * 1024),
        )(signal, rows_first, rows_second)

    row_spec = P(("dp", "sp"), None)
    weight_spec = P(None, "sp", None, None, None)
    return jax.shard_map(device_program, mesh=mesh, in_specs=(row_spec, weight_spec, weight_spec), out_specs=row_spec, check_vma=False)
```

```python
import functools

import jax
import jax.numpy as jnp
from jax import lax
from jax.experimental import pallas as pl
from jax.experimental.pallas import tpu as pltpu
from jax.sharding import PartitionSpec as P

MESH = pl.DeviceIdType.MESH
CHUNKS = 20
UNROLL = 8
RING = 4
LAG_PASS1, LAG_FAST1, LAG_NEAR, LAG_FAST2, LAG_PASS2, LAG_SLOW2 = 1, 2, 3, 4, 5, 6
AHEAD = 2
SLOW1_IN, SLOW1_OUT, FAST1_IN, FAST1_OUT, FAST2_IN, FAST2_OUT, SLOW2_IN, SLOW2_OUT = range(8)


def gelu(x):
    return 0.5 * x * (1.0 + lax.erf(x * (0.5 ** 0.5)))


def at_block(block, ref):
    return (block,) if len(ref.shape) == 3 else (block // ref.shape[1], block % ref.shape[1])


def stage(src, dst, weights, s, dist, activate=False):
    blocks, rows = 1, src.shape[-2]
    for extent in src.shape[:-2]:
        blocks *= extent

    def pairs(group, carry):
        for member in range(UNROLL):
            pair = group * UNROLL + member
            low = (pair // dist) * (2 * dist) + pair % dist
            high = low + dist
            mat = jnp.concatenate([weights[(s,) + at_block(low, weights.at[s])], weights[(s,) + at_block(high, weights.at[s])]], axis=0)
            act = jnp.concatenate([src[at_block(low, src)], src[at_block(high, src)]], axis=0)
            mixed = jnp.dot(mat, act, preferred_element_type=jnp.float32).astype(jnp.bfloat16)
            if activate:
                mixed = gelu(mixed.astype(jnp.float32)).astype(jnp.bfloat16)
            dst[at_block(low, dst)] = mixed[:rows]
            dst[at_block(high, dst)] = mixed[rows:]
        return carry

    lax.fori_loop(0, blocks // 2 // UNROLL, pairs, 0)


def kernel(n, signal, rows_first, rows_second, out, pass1, pass2,
           slow1, fast1, near, fast2, slow2, ping, pong,
           slow1_w, fast1_w, near1_w, near2_w, fast2_w, slow2_w,
           send_sems, recv_sems, wsend_sems, wrecv_sems, near_sems):
    me = lax.axis_index("sp")
    fast_n = n // RING
    slow_me, fast_me = me // fast_n, me % fast_n
    chunks, width = slow1.shape[0], slow1.shape[-1]
    slow_stages, fast_stages, near_stages = slow1_w.shape[0], fast1_w.shape[0], near1_w.shape[0]
    far_stages = slow_stages + fast_stages

    near1 = pltpu.make_async_copy(rows_first.at[pl.ds(far_stages, near_stages)], near1_w, near_sems.at[0])
    near2 = pltpu.make_async_copy(rows_second.at[pl.ds(0, near_stages)], near2_w, near_sems.at[1])
    near1.start()
    near2.start()

    def slow_peer(k):
        other = lax.rem(slow_me + k, RING)
        return other, other * fast_n + fast_me

    def fast_peer(k):
        other = lax.rem(fast_me + k, fast_n)
        return other, slow_me * fast_n + other

    barrier = pltpu.get_barrier_semaphore()
    for count, peer in ((RING, slow_peer), (fast_n, fast_peer)):
        for k in range(1, count):
            pl.semaphore_signal(barrier, inc=1, device_id={"sp": peer(k)[1]}, device_id_type=MESH)
    pl.semaphore_wait(barrier, RING + fast_n - 2)

    def spread(peer, count, src_of, dst, send_sem, recv_sem):
        for k in range(1, count):
            other, device = peer(k)
            pltpu.make_async_remote_copy(
                src_ref=src_of(other), dst_ref=dst, send_sem=send_sem, recv_sem=recv_sem,
                device_id={"sp": device}, device_id_type=MESH).start()

    def spread_slow(src_of, dst, send_sem, recv_sem):
        spread(slow_peer, RING, src_of, dst, send_sem, recv_sem)
        pltpu.make_async_copy(src_of(slow_me), dst, recv_sem).start()

    def spread_fast(src_of, dst, send_sem, recv_sem, own_copy=True):
        spread(fast_peer, fast_n, src_of, dst, send_sem, recv_sem)
        if own_copy:
            pltpu.make_async_copy(src_of(fast_me), dst, recv_sem).start()

    def wait_bytes(ref, sem):
        pltpu.make_async_copy(ref, ref, sem).wait()

    def sems(kind, chunk):
        return send_sems.at[kind, chunk], recv_sems.at[kind, chunk]

    def columns_of(chunk):
        return pl.ds(pl.multiple_of(chunk * width, width), width)

    def run(buf, steps):
        last = len(steps) - 1
        for i, (weights, s, dist, activate) in enumerate(steps):
            stage(buf if i == 0 else (ping, pong)[(i - 1) % 2], buf if i == last else (ping, pong)[i % 2], weights, s, dist, activate)

    def start_chunk(chunk):
        spread_slow(lambda other: signal.at[other, :, :, columns_of(chunk)], slow1.at[chunk, slow_me], *sems(SLOW1_IN, chunk))

    def do_slow1(chunk):
        wait_bytes(slow1.at[chunk], recv_sems.at[SLOW1_IN, chunk])
        run(slow1.at[chunk], [(slow1_w, s, 2 ** (near_stages - 1 - s), False) for s in range(slow_stages)])
        spread_slow(lambda other: slow1.at[chunk, other], pass1.at[chunk, slow_me], *sems(SLOW1_OUT, chunk))

    def do_pass1(chunk):
        wait_bytes(pass1.at[chunk], recv_sems.at[SLOW1_OUT, chunk])
        spread_fast(lambda other: pass1.at[chunk, :, other], fast1.at[chunk, fast_me], *sems(FAST1_IN, chunk))

    def do_fast1(chunk):
        wait_bytes(fast1.at[chunk], recv_sems.at[FAST1_IN, chunk])
        run(fast1.at[chunk], [(fast1_w, s, 2 ** (near_stages - 1 - s), False) for s in range(fast_stages)])
        spread_fast(lambda other: fast1.at[chunk, other], near.at[chunk, :, fast_me], *sems(FAST1_OUT, chunk), own_copy=False)
        for i in range(RING):
            near[chunk, i, fast_me] = fast1[chunk, fast_me, i]

    def do_near(chunk):
        wait_bytes(fast1.at[chunk, pl.ds(0, fast_n - 1)], recv_sems.at[FAST1_OUT, chunk])
        run(near.at[chunk],
            [(near1_w, s, 2 ** (near_stages - 1 - s), s == near_stages - 1) for s in range(near_stages)]
            + [(near2_w, s, 2 ** s, False) for s in range(near_stages)])
        spread_fast(lambda other: near.at[chunk, :, other], fast2.at[chunk, fast_me], *sems(FAST2_IN, chunk), own_copy=False)
        for i in range(RING):
            fast2[chunk, fast_me, i] = near[chunk, i, fast_me]

    def do_fast2(chunk):
        wait_bytes(fast2.at[chunk, pl.ds(0, fast_n - 1)], recv_sems.at[FAST2_IN, chunk])
        run(fast2.at[chunk], [(fast2_w, s, 2 ** (near_stages - fast_stages + s), False) for s in range(fast_stages)])
        spread_fast(lambda other: fast2.at[chunk, other], pass2.at[chunk, :, fast_me], *sems(FAST2_OUT, chunk))

    def do_pass2(chunk):
        wait_bytes(pass2.at[chunk], recv_sems.at[FAST2_OUT, chunk])
        spread_slow(lambda other: pass2.at[chunk, other], slow2.at[chunk, slow_me], *sems(SLOW2_IN, chunk))

    def do_slow2(chunk):
        wait_bytes(slow2.at[chunk], recv_sems.at[SLOW2_IN, chunk])
        run(slow2.at[chunk], [(slow2_w, s, 2 ** (near_stages - slow_stages + s), False) for s in range(slow_stages)])
        spread_slow(lambda other: slow2.at[chunk, other], out.at[slow_me, :, :, columns_of(chunk)], *sems(SLOW2_OUT, chunk))

    def slow_weights(rows, base, dst, slot):
        spread_slow(lambda other: rows.at[pl.ds(base, slow_stages), other], dst.at[:, slow_me], wsend_sems.at[slot], wrecv_sems.at[slot])

    def fast_weights(rows, base, dst, slot):
        spread_fast(lambda other: rows.at[pl.ds(base, fast_stages), :, other], dst.at[:, fast_me], wsend_sems.at[slot], wrecv_sems.at[slot])

    slow_weights(rows_first, 0, slow1_w, 0)
    for chunk in range(AHEAD):
        start_chunk(chunk)
    fast_weights(rows_first, slow_stages, fast1_w, 1)
    wait_bytes(slow1_w, wrecv_sems.at[0])

    def slot(t, carry):
        def step(lag, work):
            @pl.when(jnp.logical_and(t >= lag, t - lag < chunks))
            def _():
                work(t - lag)

        @pl.when(t == 1)
        def _():
            fast_weights(rows_second, near_stages, fast2_w, 2)
            slow_weights(rows_second, near_stages + fast_stages, slow2_w, 3)

        @pl.when(t == LAG_SLOW2)
        def _():
            wait_bytes(slow2_w, wrecv_sems.at[3])

        step(LAG_SLOW2, do_slow2)
        step(LAG_PASS2, do_pass2)

        @pl.when(t == LAG_FAST2)
        def _():
            wait_bytes(fast2_w, wrecv_sems.at[2])

        step(LAG_FAST2, do_fast2)

        @pl.when(t == LAG_NEAR)
        def _():
            wait_bytes(near1_w, near_sems.at[0])
            wait_bytes(near2_w, near_sems.at[1])

        step(LAG_NEAR, do_near)

        @pl.when(t == LAG_FAST1)
        def _():
            wait_bytes(fast1_w, wrecv_sems.at[1])

        step(LAG_FAST1, do_fast1)
        step(LAG_PASS1, do_pass1)
        step(0, do_slow1)

        @pl.when(t + AHEAD < chunks)
        def _():
            start_chunk(t + AHEAD)

        return carry

    lax.fori_loop(0, chunks + LAG_SLOW2, slot, 0)

    def finish(chunk, carry):
        wait_bytes(out.at[:, :, :, columns_of(chunk)], recv_sems.at[SLOW2_OUT, chunk])
        for kind in (SLOW1_IN, SLOW1_OUT, SLOW2_IN, SLOW2_OUT):
            wait_bytes(slow1.at[chunk, pl.ds(0, RING - 1)], send_sems.at[kind, chunk])
        for kind in (FAST1_IN, FAST1_OUT, FAST2_IN, FAST2_OUT):
            wait_bytes(fast1.at[chunk, pl.ds(0, fast_n - 1)], send_sems.at[kind, chunk])
        return carry

    lax.fori_loop(0, chunks, finish, 0)
    for slot_id, ref in ((0, slow1_w.at[:, pl.ds(0, RING - 1)]), (1, fast1_w.at[:, pl.ds(0, fast_n - 1)]),
                         (2, fast1_w.at[:, pl.ds(0, fast_n - 1)]), (3, slow1_w.at[:, pl.ds(0, RING - 1)])):
        wait_bytes(ref, wsend_sems.at[slot_id])


def weight_rows_kernel(distances, weights, rows):
    blocks, _, size, _ = weights.shape
    s = pl.program_id(0)
    base = lax.axis_index("sp") * blocks
    dist = distances[0]
    for i, value in enumerate(distances):
        dist = jnp.where(s == i, value, dist)

    def one(block, carry):
        upper = ((base + block) // dist) % 2
        rows[block] = jnp.concatenate([weights[block, upper], weights[block, 1 - upper]], axis=-1)
        return carry

    lax.fori_loop(0, blocks, one, 0, unroll=4)


def solution(mesh):
    n = mesh.shape["sp"]

    def weight_rows(weights, distances):
        stages, blocks, two, size, _ = weights.shape
        return pl.pallas_call(
            functools.partial(weight_rows_kernel, distances),
            grid=(stages,),
            out_shape=jax.ShapeDtypeStruct((stages, blocks, size, 2 * size), weights.dtype),
            in_specs=[pl.BlockSpec((None, blocks, two, size, size), lambda s: (s, 0, 0, 0, 0))],
            out_specs=pl.BlockSpec((None, blocks, size, 2 * size), lambda s: (s, 0, 0, 0)),
        )(weights)

    def device_program(signal, w_first, w_second):
        stages, blocks, _, size, _ = w_first.shape
        near_stages = stages // 2
        fast_n, inner = n // RING, blocks // RING
        slow_stages = RING.bit_length() - 1
        fast_stages = near_stages - slow_stages
        width = signal.shape[1] // CHUNKS
        dist_down = [2 ** (stages - 1 - level) for level in range(stages)]
        split = (stages, RING, inner, size, 2 * size)
        rows_first = weight_rows(w_first, dist_down).reshape(split)
        rows_second = weight_rows(w_second, dist_down[::-1]).reshape(split)
        bf16 = jnp.bfloat16
        by_slow = (CHUNKS, RING, inner, size, width)
        by_fast = (CHUNKS, fast_n, blocks // fast_n, size, width)
        half = pltpu.VMEM((blocks, size, width), bf16)

        def mats(count, outer):
            return pltpu.VMEM((count, outer, blocks // outer, size, 2 * size), bf16)

        shaped = signal.reshape(RING, inner, size, signal.shape[1])
        result = pl.pallas_call(
            functools.partial(kernel, n),
            out_shape=[jax.ShapeDtypeStruct(shaped.shape, bf16), jax.ShapeDtypeStruct(by_slow, bf16), jax.ShapeDtypeStruct(by_slow, bf16)],
            in_specs=[pl.BlockSpec(memory_space=pl.ANY)] * 3,
            out_specs=[pl.BlockSpec(memory_space=pl.ANY)] * 3,
            scratch_shapes=[
                pltpu.VMEM(by_slow, bf16), pltpu.VMEM(by_fast, bf16), pltpu.VMEM(by_slow, bf16), pltpu.VMEM(by_fast, bf16), pltpu.VMEM(by_slow, bf16),
                half, half,
                mats(slow_stages, RING), mats(fast_stages, fast_n), mats(near_stages, RING), mats(near_stages, RING), mats(fast_stages, fast_n), mats(slow_stages, RING),
                pltpu.SemaphoreType.DMA((8, CHUNKS)), pltpu.SemaphoreType.DMA((8, CHUNKS)),
                pltpu.SemaphoreType.DMA((4,)), pltpu.SemaphoreType.DMA((4,)), pltpu.SemaphoreType.DMA((2,))],
            compiler_params=pltpu.CompilerParams(collective_id=0, has_side_effects=True, vmem_limit_bytes=67043328),
        )(shaped, rows_first, rows_second)
        return result[0].reshape(signal.shape)

    row_spec = P(("dp", "sp"), None)
    weight_spec = P(None, "sp", None, None, None)
    return jax.shard_map(device_program, mesh=mesh, in_specs=(row_spec, weight_spec, weight_spec), out_specs=row_spec, check_vma=False)
```

```python
import functools

import jax
import jax.numpy as jnp
from jax import lax
from jax.experimental import pallas as pl
from jax.experimental.pallas import tpu as pltpu
from jax.sharding import PartitionSpec as P

MESH = pl.DeviceIdType.MESH
CHUNKS = 20
UNROLL = 8
PIECES = 4
ROWS_UNROLL = 4
RING = 4
LAG_PASS1, LAG_FAST1, LAG_NEAR, LAG_FAST2, LAG_PASS2, LAG_SLOW2 = 1, 2, 3, 4, 5, 6
AHEAD = 2
SLOW1_IN, SLOW1_OUT, FAST1_IN, FAST1_OUT, FAST2_IN, FAST2_OUT, SLOW2_IN, SLOW2_OUT = range(8)


def gelu(x):
    return 0.5 * x * (1.0 + lax.erf(x * (0.5 ** 0.5)))


def at_block(block, ref):
    return (block,) if len(ref.shape) == 3 else (block // ref.shape[1], block % ref.shape[1])


def stage(src, dst, weights, s, dist, activate=False):
    blocks, rows = 1, src.shape[-2]
    for extent in src.shape[:-2]:
        blocks *= extent

    def pairs(group, carry):
        for member in range(UNROLL):
            pair = group * UNROLL + member
            low = (pair // dist) * (2 * dist) + pair % dist
            high = low + dist
            mat = jnp.concatenate([weights[(s,) + at_block(low, weights.at[s])], weights[(s,) + at_block(high, weights.at[s])]], axis=0)
            act = jnp.concatenate([src[at_block(low, src)], src[at_block(high, src)]], axis=0)
            mixed = jnp.dot(mat, act, preferred_element_type=jnp.float32).astype(jnp.bfloat16)
            if activate:
                mixed = gelu(mixed.astype(jnp.float32)).astype(jnp.bfloat16)
            dst[at_block(low, dst)] = mixed[:rows]
            dst[at_block(high, dst)] = mixed[rows:]
        return carry

    lax.fori_loop(0, blocks // 2 // UNROLL, pairs, 0)


def kernel(n, signal, w_first, w_second, out, pass1, pass2,
           slow1, fast1, near, fast2, slow2, ping, pong,
           slow1_w, fast1_w, near1_w, near2_w, fast2_w, slow2_w,
           raw, send_sems, recv_sems, wsend_sems, wrecv_sems, raw_sems, credit_sem):
    me = lax.axis_index("sp")
    fast_n = n // RING
    slow_me, fast_me = me // fast_n, me % fast_n
    chunks, width = slow1.shape[0], slow1.shape[-1]
    slow_stages, fast_stages, near_stages = slow1_w.shape[0], fast1_w.shape[0], near1_w.shape[0]
    far_stages = slow_stages + fast_stages

    def slow_peer(k):
        other = lax.rem(slow_me + k, RING)
        return other, other * fast_n + fast_me

    def fast_peer(k):
        other = lax.rem(fast_me + k, fast_n)
        return other, slow_me * fast_n + other

    barrier = pltpu.get_barrier_semaphore()
    for count, peer in ((RING, slow_peer), (fast_n, fast_peer)):
        for k in range(1, count):
            pl.semaphore_signal(barrier, inc=1, device_id={"sp": peer(k)[1]}, device_id_type=MESH)
    pl.semaphore_wait(barrier, RING + fast_n - 2)

    def spread(peer, count, src_of, dst, send_sem, recv_sem):
        for k in range(1, count):
            other, device = peer(k)
            pltpu.make_async_remote_copy(
                src_ref=src_of(other), dst_ref=dst, send_sem=send_sem, recv_sem=recv_sem,
                device_id={"sp": device}, device_id_type=MESH).start()

    def spread_slow(src_of, dst, send_sem, recv_sem):
        spread(slow_peer, RING, src_of, dst, send_sem, recv_sem)
        pltpu.make_async_copy(src_of(slow_me), dst, recv_sem).start()

    def spread_fast(src_of, dst, send_sem, recv_sem, own_copy=True):
        spread(fast_peer, fast_n, src_of, dst, send_sem, recv_sem)
        if own_copy:
            pltpu.make_async_copy(src_of(fast_me), dst, recv_sem).start()

    def wait_bytes(ref, sem):
        pltpu.make_async_copy(ref, ref, sem).wait()

    def sems(kind, chunk):
        return send_sems.at[kind, chunk], recv_sems.at[kind, chunk]

    def columns_of(chunk):
        return pl.ds(pl.multiple_of(chunk * width, width), width)

    def run(buf, steps):
        last = len(steps) - 1
        for i, (weights, s, dist, activate) in enumerate(steps):
            stage(buf if i == 0 else (ping, pong)[(i - 1) % 2], buf if i == last else (ping, pong)[i % 2], weights, s, dist, activate)

    def start_chunk(chunk):
        spread_slow(lambda other: signal.at[other, :, :, columns_of(chunk)], slow1.at[chunk, slow_me], *sems(SLOW1_IN, chunk))

    def do_slow1(chunk):
        wait_bytes(slow1.at[chunk], recv_sems.at[SLOW1_IN, chunk])
        run(slow1.at[chunk], [(slow1_w, s, 2 ** (near_stages - 1 - s), False) for s in range(slow_stages)])
        spread_slow(lambda other: slow1.at[chunk, other], pass1.at[chunk, slow_me], *sems(SLOW1_OUT, chunk))

    def do_pass1(chunk):
        wait_bytes(pass1.at[chunk], recv_sems.at[SLOW1_OUT, chunk])
        spread_fast(lambda other: pass1.at[chunk, :, other], fast1.at[chunk, fast_me], *sems(FAST1_IN, chunk))

    def do_fast1(chunk):
        wait_bytes(fast1.at[chunk], recv_sems.at[FAST1_IN, chunk])
        run(fast1.at[chunk], [(fast1_w, s, 2 ** (near_stages - 1 - s), False) for s in range(fast_stages)])
        spread_fast(lambda other: fast1.at[chunk, other], near.at[chunk, :, fast_me], *sems(FAST1_OUT, chunk), own_copy=False)
        for i in range(RING):
            near[chunk, i, fast_me] = fast1[chunk, fast_me, i]

    def do_near(chunk):
        wait_bytes(fast1.at[chunk, pl.ds(0, fast_n - 1)], recv_sems.at[FAST1_OUT, chunk])
        run(near.at[chunk],
            [(near1_w, s, 2 ** (near_stages - 1 - s), s == near_stages - 1) for s in range(near_stages)]
            + [(near2_w, s, 2 ** s, False) for s in range(near_stages)])
        spread_fast(lambda other: near.at[chunk, :, other], fast2.at[chunk, fast_me], *sems(FAST2_IN, chunk), own_copy=False)
        for i in range(RING):
            fast2[chunk, fast_me, i] = near[chunk, i, fast_me]

    def do_fast2(chunk):
        wait_bytes(fast2.at[chunk, pl.ds(0, fast_n - 1)], recv_sems.at[FAST2_IN, chunk])
        run(fast2.at[chunk], [(fast2_w, s, 2 ** (near_stages - fast_stages + s), False) for s in range(fast_stages)])
        spread_fast(lambda other: fast2.at[chunk, other], pass2.at[chunk, :, fast_me], *sems(FAST2_OUT, chunk))

    def do_pass2(chunk):
        wait_bytes(pass2.at[chunk], recv_sems.at[FAST2_OUT, chunk])
        spread_slow(lambda other: pass2.at[chunk, other], slow2.at[chunk, slow_me], *sems(SLOW2_IN, chunk))

    def do_slow2(chunk):
        wait_bytes(slow2.at[chunk], recv_sems.at[SLOW2_IN, chunk])
        run(slow2.at[chunk], [(slow2_w, s, 2 ** (near_stages - slow_stages + s), False) for s in range(slow_stages)])
        spread_slow(lambda other: slow2.at[chunk, other], out.at[slow_me, :, :, columns_of(chunk)], *sems(SLOW2_OUT, chunk))

    half_blocks = raw.shape[1]
    own_block = me * (2 * half_blocks)

    def weight_rows(weights, base, count, level, growing, put):
        def load(s, p):
            slot = (2 * s + p) % PIECES
            return pltpu.make_async_copy(weights.at[base + s, pl.ds(p * half_blocks, half_blocks)], raw.at[slot], raw_sems.at[slot])

        for s in range(PIECES // 2):
            for p in range(2):
                load(s, p).start()

        for s in range(count):
            dist = 2 ** (level + s if growing else level - s)

            def piece(p, carry, s=s, dist=dist):
                load(s, p).wait()
                slot = (2 * s + p) % PIECES

                def group(g, carry):
                    for k in range(ROWS_UNROLL):
                        member = g * ROWS_UNROLL + k
                        block = p * half_blocks + member
                        upper = ((own_block + block) // dist) % 2
                        put(s, block, jnp.concatenate([raw[slot, member, upper], raw[slot, member, 1 - upper]], axis=-1))
                    return carry

                lax.fori_loop(0, half_blocks // ROWS_UNROLL, group, 0)
                if s + PIECES // 2 < count:
                    load(s + PIECES // 2, p).start()
                return carry

            lax.fori_loop(0, 2, piece, 0)

    def into(ref, first):
        def put(s, block, value):
            ref[first + s, block // ref.shape[2], block % ref.shape[2]] = value
        return put

    def slow_weights(first, dst, slot):
        spread(slow_peer, RING, lambda other: slow2.at[pl.ds(first, slow_stages), other], dst.at[:, slow_me], wsend_sems.at[slot], wrecv_sems.at[slot])
        for s in range(slow_stages):
            for i in range(dst.shape[2]):
                dst[s, slow_me, i] = slow2[first + s, slow_me, i]

    def fast_weights(first, dst, slot):
        spread(fast_peer, fast_n, lambda other: slow2.at[pl.ds(first, fast_stages), :, other], dst.at[:, fast_me], wsend_sems.at[slot], wrecv_sems.at[slot])
        for s in range(fast_stages):
            for i in range(dst.shape[2]):
                dst[s, fast_me, i] = slow2[first + s, i, fast_me]

    top = far_stages + near_stages - 1
    start_chunk(0)
    weight_rows(w_first, 0, slow_stages, top, False, into(slow2, 0))
    slow_weights(0, slow1_w, 0)
    for chunk in range(1, AHEAD):
        start_chunk(chunk)
    weight_rows(w_first, slow_stages, fast_stages, top - slow_stages, False, into(slow2, slow_stages))
    fast_weights(slow_stages, fast1_w, 1)
    weight_rows(w_second, near_stages, fast_stages, near_stages, True, into(slow2, far_stages))
    fast_weights(far_stages, fast2_w, 2)
    wait_bytes(slow1_w.at[:, pl.ds(0, RING - 1)], wrecv_sems.at[0])

    def slot(t, carry):
        def step(lag, work):
            @pl.when(jnp.logical_and(t >= lag, t - lag < chunks))
            def _():
                work(t - lag)

        @pl.when(t == LAG_PASS2 - 1)
        def _():
            for slot_id in range(4):
                wait_bytes((slow1_w.at[:, pl.ds(0, RING - 1)], fast1_w.at[:, pl.ds(0, fast_n - 1)])[slot_id in (1, 2)], wsend_sems.at[slot_id])
            for k in range(1, RING):
                pl.semaphore_signal(credit_sem, inc=1, device_id={"sp": slow_peer(k)[1]}, device_id_type=MESH)

        @pl.when(t == LAG_SLOW2)
        def _():
            wait_bytes(slow2_w.at[:, pl.ds(0, RING - 1)], wrecv_sems.at[3])

        step(LAG_SLOW2, do_slow2)

        @pl.when(t == LAG_PASS2)
        def _():
            pl.semaphore_wait(credit_sem, RING - 1)

        step(LAG_PASS2, do_pass2)

        @pl.when(t == LAG_FAST2)
        def _():
            wait_bytes(fast2_w.at[:, pl.ds(0, fast_n - 1)], wrecv_sems.at[2])

        step(LAG_FAST2, do_fast2)
        step(LAG_NEAR, do_near)

        @pl.when(t == LAG_FAST1)
        def _():
            wait_bytes(fast1_w.at[:, pl.ds(0, fast_n - 1)], wrecv_sems.at[1])

        step(LAG_FAST1, do_fast1)
        step(LAG_PASS1, do_pass1)
        step(0, do_slow1)

        @pl.when(t + AHEAD < chunks)
        def _():
            start_chunk(t + AHEAD)

        @pl.when(t == 0)
        def _():
            weight_rows(w_first, far_stages, near_stages, top - far_stages, False, into(near1_w, 0))

        @pl.when(t == 1)
        def _():
            weight_rows(w_second, 0, near_stages, 0, True, into(near2_w, 0))

        @pl.when(t == 2)
        def _():
            weight_rows(w_second, near_stages + fast_stages, slow_stages, near_stages + fast_stages, True, into(slow2, far_stages + fast_stages))
            slow_weights(far_stages + fast_stages, slow2_w, 3)

        return carry

    lax.fori_loop(0, chunks + LAG_SLOW2, slot, 0)

    def finish(chunk, carry):
        wait_bytes(out.at[:, :, :, columns_of(chunk)], recv_sems.at[SLOW2_OUT, chunk])
        for kind in (SLOW1_IN, SLOW1_OUT, SLOW2_IN, SLOW2_OUT):
            wait_bytes(slow1.at[chunk, pl.ds(0, RING - 1)], send_sems.at[kind, chunk])
        for kind in (FAST1_IN, FAST1_OUT, FAST2_IN, FAST2_OUT):
            wait_bytes(fast1.at[chunk, pl.ds(0, fast_n - 1)], send_sems.at[kind, chunk])
        return carry

    lax.fori_loop(0, chunks, finish, 0)


def solution(mesh):
    n = mesh.shape["sp"]

    def device_program(signal, w_first, w_second):
        stages, blocks, _, size, _ = w_first.shape
        near_stages = stages // 2
        fast_n, inner = n // RING, blocks // RING
        slow_stages = RING.bit_length() - 1
        fast_stages = near_stages - slow_stages
        width = signal.shape[1] // CHUNKS
        bf16 = jnp.bfloat16
        by_slow = (CHUNKS, RING, inner, size, width)
        by_fast = (CHUNKS, fast_n, blocks // fast_n, size, width)
        half = pltpu.VMEM((blocks, size, width), bf16)

        def mats(count, outer):
            return pltpu.VMEM((count, outer, blocks // outer, size, 2 * size), bf16)

        shaped = signal.reshape(RING, inner, size, signal.shape[1])
        result = pl.pallas_call(
            functools.partial(kernel, n),
            out_shape=[jax.ShapeDtypeStruct(shaped.shape, bf16), jax.ShapeDtypeStruct(by_slow, bf16), jax.ShapeDtypeStruct(by_slow, bf16)],
            in_specs=[pl.BlockSpec(memory_space=pl.ANY)] * 3,
            out_specs=[pl.BlockSpec(memory_space=pl.ANY)] * 3,
            scratch_shapes=[
                pltpu.VMEM(by_slow, bf16), pltpu.VMEM(by_fast, bf16), pltpu.VMEM(by_slow, bf16), pltpu.VMEM(by_fast, bf16), pltpu.VMEM(by_slow, bf16),
                half, half,
                mats(slow_stages, RING), mats(fast_stages, fast_n), mats(near_stages, RING), mats(near_stages, RING), mats(fast_stages, fast_n), mats(slow_stages, RING),
                pltpu.VMEM((PIECES, blocks // 2, 2, size, size), bf16),
                pltpu.SemaphoreType.DMA((8, CHUNKS)), pltpu.SemaphoreType.DMA((8, CHUNKS)),
                pltpu.SemaphoreType.DMA((4,)), pltpu.SemaphoreType.DMA((4,)), pltpu.SemaphoreType.DMA((PIECES,)), pltpu.SemaphoreType.REGULAR],
            compiler_params=pltpu.CompilerParams(collective_id=0, has_side_effects=True, vmem_limit_bytes=67043328),
        )(shaped, w_first, w_second)
        return result[0].reshape(signal.shape)

    row_spec = P(("dp", "sp"), None)
    weight_spec = P(None, "sp", None, None, None)
    return jax.shard_map(device_program, mesh=mesh, in_specs=(row_spec, weight_spec, weight_spec), out_specs=row_spec, check_vma=False)
```

```python
import functools

import jax
import jax.numpy as jnp
from jax import lax
from jax.experimental import pallas as pl
from jax.experimental.pallas import tpu as pltpu
from jax.sharding import PartitionSpec as P

MESH = pl.DeviceIdType.MESH
CHUNKS = 20
UNROLL = 16
PIECES = 4
ROWS_UNROLL = 8
RING = 4
LAG_PASS1, LAG_FAST1, LAG_NEAR, LAG_FAST2, LAG_PASS2, LAG_SLOW2 = 1, 2, 3, 4, 5, 6
AHEAD = 2
SLOW1_IN, SLOW1_OUT, FAST1_IN, FAST1_OUT, FAST2_IN, FAST2_OUT, SLOW2_IN, SLOW2_OUT = range(8)


def gelu(x):
    return 0.5 * x * (1.0 + lax.erf(x * (0.5 ** 0.5)))


def at_block(block, ref):
    return (block,) if len(ref.shape) == 3 else (lax.div(block, ref.shape[1]), lax.rem(block, ref.shape[1]))


def stage(src, dst, weights, s, dist, activate=False):
    blocks, rows = 1, src.shape[-2]
    for extent in src.shape[:-2]:
        blocks *= extent

    def pairs(group, carry):
        for member in range(UNROLL):
            pair = group * UNROLL + member
            low = lax.div(pair, dist) * (2 * dist) + lax.rem(pair, dist)
            high = low + dist
            mat = jnp.concatenate([weights[(s,) + at_block(low, weights.at[s])], weights[(s,) + at_block(high, weights.at[s])]], axis=0)
            act = jnp.concatenate([src[at_block(low, src)], src[at_block(high, src)]], axis=0)
            mixed = jnp.dot(mat, act, preferred_element_type=jnp.float32).astype(jnp.bfloat16)
            if activate:
                mixed = gelu(mixed.astype(jnp.float32)).astype(jnp.bfloat16)
            dst[at_block(low, dst)] = mixed[:rows]
            dst[at_block(high, dst)] = mixed[rows:]
        return carry

    lax.fori_loop(0, blocks // 2 // UNROLL, pairs, 0)


def kernel(n, signal, w_first, w_second, out, pass1, pass2,
           slow1, fast1, near, fast2, slow2, ping, pong,
           slow1_w, fast1_w, near1_w, near2_w, fast2_w, slow2_w,
           raw, send_sems, recv_sems, wsend_sems, wrecv_sems, raw_sems, credit_sem):
    me = lax.axis_index("sp")
    fast_n = n // RING
    slow_me, fast_me = lax.div(me, fast_n), lax.rem(me, fast_n)
    chunks, width = slow1.shape[0], slow1.shape[-1]
    slow_stages, fast_stages, near_stages = slow1_w.shape[0], fast1_w.shape[0], near1_w.shape[0]
    far_stages = slow_stages + fast_stages

    def slow_peer(k):
        other = lax.rem(slow_me + k, RING)
        return other, other * fast_n + fast_me

    def fast_peer(k):
        other = lax.rem(fast_me + k, fast_n)
        return other, slow_me * fast_n + other

    barrier = pltpu.get_barrier_semaphore()
    for count, peer in ((RING, slow_peer), (fast_n, fast_peer)):
        for k in range(1, count):
            pl.semaphore_signal(barrier, inc=1, device_id={"sp": peer(k)[1]}, device_id_type=MESH)
    pl.semaphore_wait(barrier, RING + fast_n - 2)

    def spread(peer, count, src_of, dst, send_sem, recv_sem):
        for k in range(1, count):
            other, device = peer(k)
            pltpu.make_async_remote_copy(
                src_ref=src_of(other), dst_ref=dst, send_sem=send_sem, recv_sem=recv_sem,
                device_id={"sp": device}, device_id_type=MESH).start()

    def spread_slow(src_of, dst, send_sem, recv_sem):
        spread(slow_peer, RING, src_of, dst, send_sem, recv_sem)
        pltpu.make_async_copy(src_of(slow_me), dst, recv_sem).start()

    def spread_fast(src_of, dst, send_sem, recv_sem, own_copy=True):
        spread(fast_peer, fast_n, src_of, dst, send_sem, recv_sem)
        if own_copy:
            pltpu.make_async_copy(src_of(fast_me), dst, recv_sem).start()

    def wait_bytes(ref, sem):
        pltpu.make_async_copy(ref, ref, sem).wait()

    def sems(kind, chunk):
        return send_sems.at[kind, chunk], recv_sems.at[kind, chunk]

    def columns_of(chunk):
        return pl.ds(pl.multiple_of(chunk * width, width), width)

    def run(buf, steps):
        last = len(steps) - 1
        for i, (weights, s, dist, activate) in enumerate(steps):
            stage(buf if i == 0 else (ping, pong)[(i - 1) % 2], buf if i == last else (ping, pong)[i % 2], weights, s, dist, activate)

    def start_chunk(chunk):
        spread_slow(lambda other: signal.at[other, :, :, columns_of(chunk)], slow1.at[chunk, slow_me], *sems(SLOW1_IN, chunk))

    def do_slow1(chunk):
        wait_bytes(slow1.at[chunk], recv_sems.at[SLOW1_IN, chunk])
        run(slow1.at[chunk], [(slow1_w, s, 2 ** (near_stages - 1 - s), False) for s in range(slow_stages)])
        spread_slow(lambda other: slow1.at[chunk, other], pass1.at[chunk, slow_me], *sems(SLOW1_OUT, chunk))

    def do_pass1(chunk):
        wait_bytes(pass1.at[chunk], recv_sems.at[SLOW1_OUT, chunk])
        spread_fast(lambda other: pass1.at[chunk, :, other], fast1.at[chunk, fast_me], *sems(FAST1_IN, chunk))

    def do_fast1(chunk):
        wait_bytes(fast1.at[chunk], recv_sems.at[FAST1_IN, chunk])
        run(fast1.at[chunk], [(fast1_w, s, 2 ** (near_stages - 1 - s), False) for s in range(fast_stages)])
        spread_fast(lambda other: fast1.at[chunk, other], near.at[chunk, :, fast_me], *sems(FAST1_OUT, chunk), own_copy=False)
        for i in range(RING):
            near[chunk, i, fast_me] = fast1[chunk, fast_me, i]

    def do_near(chunk):
        wait_bytes(fast1.at[chunk, pl.ds(0, fast_n - 1)], recv_sems.at[FAST1_OUT, chunk])
        run(near.at[chunk],
            [(near1_w, s, 2 ** (near_stages - 1 - s), s == near_stages - 1) for s in range(near_stages)]
            + [(near2_w, s, 2 ** s, False) for s in range(near_stages)])
        spread_fast(lambda other: near.at[chunk, :, other], fast2.at[chunk, fast_me], *sems(FAST2_IN, chunk), own_copy=False)
        for i in range(RING):
            fast2[chunk, fast_me, i] = near[chunk, i, fast_me]

    def do_fast2(chunk):
        wait_bytes(fast2.at[chunk, pl.ds(0, fast_n - 1)], recv_sems.at[FAST2_IN, chunk])
        run(fast2.at[chunk], [(fast2_w, s, 2 ** (near_stages - fast_stages + s), False) for s in range(fast_stages)])
        spread_fast(lambda other: fast2.at[chunk, other], pass2.at[chunk, :, fast_me], *sems(FAST2_OUT, chunk))

    def do_pass2(chunk):
        wait_bytes(pass2.at[chunk], recv_sems.at[FAST2_OUT, chunk])
        spread_slow(lambda other: pass2.at[chunk, other], slow2.at[chunk, slow_me], *sems(SLOW2_IN, chunk))

    def do_slow2(chunk):
        wait_bytes(slow2.at[chunk], recv_sems.at[SLOW2_IN, chunk])
        run(slow2.at[chunk], [(slow2_w, s, 2 ** (near_stages - slow_stages + s), False) for s in range(slow_stages)])
        spread_slow(lambda other: slow2.at[chunk, other], out.at[slow_me, :, :, columns_of(chunk)], *sems(SLOW2_OUT, chunk))

    half_blocks = raw.shape[1]
    own_block = me * (2 * half_blocks)

    def weight_rows(weights, base, count, level, growing, put):
        def load(s, p):
            slot = lax.rem(2 * s + p, PIECES)
            return pltpu.make_async_copy(weights.at[base + s, pl.ds(p * half_blocks, half_blocks)], raw.at[slot], raw_sems.at[slot])

        for s in range(PIECES // 2):
            for p in range(2):
                load(s, jnp.int32(p)).start()

        for s in range(count):
            dist = 2 ** (level + s if growing else level - s)

            def piece(p, carry, s=s, dist=dist):
                load(s, p).wait()
                slot = lax.rem(2 * s + p, PIECES)

                def group(g, carry):
                    for k in range(ROWS_UNROLL):
                        member = g * ROWS_UNROLL + k
                        block = p * half_blocks + member
                        upper = lax.rem(lax.div(own_block + block, dist), 2)
                        put(s, block, jnp.concatenate([raw[slot, member, upper], raw[slot, member, 1 - upper]], axis=-1))
                    return carry

                lax.fori_loop(0, half_blocks // ROWS_UNROLL, group, 0)
                if s + PIECES // 2 < count:
                    load(s + PIECES // 2, p).start()
                return carry

            lax.fori_loop(0, 2, piece, 0)

    def into(ref, first):
        def put(s, block, value):
            ref[first + s, lax.div(block, ref.shape[2]), lax.rem(block, ref.shape[2])] = value
        return put

    def slow_weights(first, dst, slot):
        spread(slow_peer, RING, lambda other: slow2.at[pl.ds(first, slow_stages), other], dst.at[:, slow_me], wsend_sems.at[slot], wrecv_sems.at[slot])
        for s in range(slow_stages):
            for i in range(dst.shape[2]):
                dst[s, slow_me, i] = slow2[first + s, slow_me, i]

    def fast_weights(first, dst, slot):
        spread(fast_peer, fast_n, lambda other: slow2.at[pl.ds(first, fast_stages), :, other], dst.at[:, fast_me], wsend_sems.at[slot], wrecv_sems.at[slot])
        for s in range(fast_stages):
            for i in range(dst.shape[2]):
                dst[s, fast_me, i] = slow2[first + s, i, fast_me]

    top = far_stages + near_stages - 1
    start_chunk(0)
    weight_rows(w_first, 0, slow_stages, top, False, into(slow2, 0))
    slow_weights(0, slow1_w, 0)
    for chunk in range(1, AHEAD):
        start_chunk(chunk)
    weight_rows(w_first, slow_stages, fast_stages, top - slow_stages, False, into(slow2, slow_stages))
    fast_weights(slow_stages, fast1_w, 1)
    weight_rows(w_second, near_stages, fast_stages, near_stages, True, into(slow2, far_stages))
    fast_weights(far_stages, fast2_w, 2)
    wait_bytes(slow1_w.at[:, pl.ds(0, RING - 1)], wrecv_sems.at[0])

    def slot(t, carry):
        def step(lag, work):
            @pl.when(jnp.logical_and(t >= lag, t - lag < chunks))
            def _():
                work(t - lag)

        @pl.when(t == LAG_PASS2 - 1)
        def _():
            for slot_id in range(4):
                wait_bytes((slow1_w.at[:, pl.ds(0, RING - 1)], fast1_w.at[:, pl.ds(0, fast_n - 1)])[slot_id in (1, 2)], wsend_sems.at[slot_id])
            for k in range(1, RING):
                pl.semaphore_signal(credit_sem, inc=1, device_id={"sp": slow_peer(k)[1]}, device_id_type=MESH)

        @pl.when(t == LAG_SLOW2)
        def _():
            wait_bytes(slow2_w.at[:, pl.ds(0, RING - 1)], wrecv_sems.at[3])

        step(LAG_SLOW2, do_slow2)

        @pl.when(t == LAG_PASS2)
        def _():
            pl.semaphore_wait(credit_sem, RING - 1)

        step(LAG_PASS2, do_pass2)

        @pl.when(t == LAG_FAST2)
        def _():
            wait_bytes(fast2_w.at[:, pl.ds(0, fast_n - 1)], wrecv_sems.at[2])

        step(LAG_FAST2, do_fast2)
        step(LAG_NEAR, do_near)

        @pl.when(t == LAG_FAST1)
        def _():
            wait_bytes(fast1_w.at[:, pl.ds(0, fast_n - 1)], wrecv_sems.at[1])

        step(LAG_FAST1, do_fast1)
        step(LAG_PASS1, do_pass1)
        step(0, do_slow1)

        @pl.when(t + AHEAD < chunks)
        def _():
            start_chunk(t + AHEAD)

        @pl.when(t == 0)
        def _():
            weight_rows(w_first, far_stages, near_stages, top - far_stages, False, into(near1_w, 0))

        @pl.when(t == 1)
        def _():
            weight_rows(w_second, 0, near_stages, 0, True, into(near2_w, 0))

        @pl.when(t == 2)
        def _():
            weight_rows(w_second, near_stages + fast_stages, slow_stages, near_stages + fast_stages, True, into(slow2, far_stages + fast_stages))
            slow_weights(far_stages + fast_stages, slow2_w, 3)

        return carry

    lax.fori_loop(0, chunks + LAG_SLOW2, slot, 0)

    def finish(chunk, carry):
        wait_bytes(out.at[:, :, :, columns_of(chunk)], recv_sems.at[SLOW2_OUT, chunk])
        for kind in (SLOW1_IN, SLOW1_OUT, SLOW2_IN, SLOW2_OUT):
            wait_bytes(slow1.at[chunk, pl.ds(0, RING - 1)], send_sems.at[kind, chunk])
        for kind in (FAST1_IN, FAST1_OUT, FAST2_IN, FAST2_OUT):
            wait_bytes(fast1.at[chunk, pl.ds(0, fast_n - 1)], send_sems.at[kind, chunk])
        return carry

    lax.fori_loop(0, chunks, finish, 0)


def solution(mesh):
    n = mesh.shape["sp"]

    def device_program(signal, w_first, w_second):
        stages, blocks, _, size, _ = w_first.shape
        near_stages = stages // 2
        fast_n, inner = n // RING, blocks // RING
        slow_stages = RING.bit_length() - 1
        fast_stages = near_stages - slow_stages
        width = signal.shape[1] // CHUNKS
        bf16 = jnp.bfloat16
        by_slow = (CHUNKS, RING, inner, size, width)
        by_fast = (CHUNKS, fast_n, blocks // fast_n, size, width)
        half = pltpu.VMEM((blocks, size, width), bf16)

        def mats(count, outer):
            return pltpu.VMEM((count, outer, blocks // outer, size, 2 * size), bf16)

        shaped = signal.reshape(RING, inner, size, signal.shape[1])
        result = pl.pallas_call(
            functools.partial(kernel, n),
            out_shape=[jax.ShapeDtypeStruct(shaped.shape, bf16), jax.ShapeDtypeStruct(by_slow, bf16), jax.ShapeDtypeStruct(by_slow, bf16)],
            in_specs=[pl.BlockSpec(memory_space=pl.ANY)] * 3,
            out_specs=[pl.BlockSpec(memory_space=pl.ANY)] * 3,
            scratch_shapes=[
                pltpu.VMEM(by_slow, bf16), pltpu.VMEM(by_fast, bf16), pltpu.VMEM(by_slow, bf16), pltpu.VMEM(by_fast, bf16), pltpu.VMEM(by_slow, bf16),
                half, half,
                mats(slow_stages, RING), mats(fast_stages, fast_n), mats(near_stages, RING), mats(near_stages, RING), mats(fast_stages, fast_n), mats(slow_stages, RING),
                pltpu.VMEM((PIECES, blocks // 2, 2, size, size), bf16),
                pltpu.SemaphoreType.DMA((8, CHUNKS)), pltpu.SemaphoreType.DMA((8, CHUNKS)),
                pltpu.SemaphoreType.DMA((4,)), pltpu.SemaphoreType.DMA((4,)), pltpu.SemaphoreType.DMA((PIECES,)), pltpu.SemaphoreType.REGULAR],
            compiler_params=pltpu.CompilerParams(collective_id=0, has_side_effects=True, vmem_limit_bytes=67043328),
        )(shaped, w_first, w_second)
        return result[0].reshape(signal.shape)

    row_spec = P(("dp", "sp"), None)
    weight_spec = P(None, "sp", None, None, None)
    return jax.shard_map(device_program, mesh=mesh, in_specs=(row_spec, weight_spec, weight_spec), out_specs=row_spec, check_vma=False)
```
